128 devices in a mesh: rows: 8 (over z, core), cols: 4 (over x), slabs: 4 (over y).
Axes of the slice: x: 4, y: 4, z: 4, core: 2. Of those that a mesh axis runs over, the one named last changes fastest.
Arguments:
- field_now: float32 [32, 128, 512, 128], P('rows', 'cols', 'slabs'), may hold values from 0.5 to 2
- earlier: float32 [32, 128, 512, 128], P('rows', 'cols', 'slabs'), may hold values from 0.2 to 1.8
- speed_square: float32 [32, 128, 512, 128], P('rows', 'cols', 'slabs'), may hold values from 0.05 to 0.3
Outputs:
- scaled_field: float32 [32, 128, 512, 128], P('rows', 'cols', 'slabs')
- field_now_end: float32 [32, 128, 512, 128], P('rows', 'cols', 'slabs')
The draws below stay inside these ranges and needn't reach their ends.
All inputs are finite; a program needn't handle non-finite values.
Results may differ from the reference program's by a relative error of at most 0.00002.
Values sent between devices are 32-bit elements; how exact they have to be, the bound alone decides.
A program may use at most 128 MiB of HBM per device.

```python
import jax
import jax.numpy as jnp
from jax import lax

GRID_J = 32
GRID_I = 128
GRID_K = 512
MEMBERS = 128
STEPS = 3


def block_levels(rng, shape, cuts, smallest, top_value):
    level, own = 1.0, jax.random.fold_in(rng, 6)
    for position, blocks in cuts:
        steps = jnp.exp(jax.random.uniform(jax.random.fold_in(own, position), (blocks,), jnp.float32, smallest / len(cuts), top_value / len(cuts)))
        level = level * jnp.repeat(steps, shape[position] // blocks).reshape([-1 if axis == position else 1 for axis in range(len(shape))])
    return level


def setup_inputs(seed: int = 0) -> dict:
    keys = jax.random.split(jax.random.key(seed), 4)
    field_now = jnp.clip(0.5 + 1.5 * jax.random.uniform(keys[0], (GRID_J, GRID_I, GRID_K, MEMBERS), jnp.float32) ** block_levels(keys[0], (GRID_J, GRID_I, GRID_K, MEMBERS), ((0, 8), (1, 4), (2, 4)), -0.2, 0.2), 0.5, 2.0)
    earlier = jnp.clip(0.2 + 1.5999999 * jax.random.uniform(keys[1], (GRID_J, GRID_I, GRID_K, MEMBERS), jnp.float32) ** block_levels(keys[1], (GRID_J, GRID_I, GRID_K, MEMBERS), ((0, 8), (1, 4), (2, 4)), -0.2, 0.2), 0.2, 1.8)
    speed_square = jnp.clip(0.05 + 0.25 * jax.random.uniform(keys[2], (GRID_J, GRID_I, GRID_K, MEMBERS), jnp.float32) ** block_levels(keys[2], (GRID_J, GRID_I, GRID_K, MEMBERS), ((0, 8), (1, 4), (2, 4)), -0.2, 0.2), 0.05, 0.3)
    return {"field_now": field_now, "earlier": earlier, "speed_square": speed_square}


def without_rim(values, dims):
    for dim in dims:
        values = lax.slice_in_dim(values, 1, values.shape[dim] - 1, axis=dim)
    return values

def shifted_cells(values, dim, start, dims):
    others = [other for other in dims if other != dim]
    values = without_rim(values, others)
    return lax.slice_in_dim(values, start, start + values.shape[dim] - 2, axis=dim)

def march_step(padded, before, speed_square):
    middle = without_rim(padded, (0, 1, 2))
    lower = [shifted_cells(padded, dim, 0, (0, 1, 2)) for dim in (0, 1, 2)]
    upper = [shifted_cells(padded, dim, 2, (0, 1, 2)) for dim in (0, 1, 2)]
    spread = lower[0] + upper[0] + lower[1] + upper[1] + lower[2] + upper[2] - 6.0 * middle
    return 2.0 * middle - before + speed_square * spread

def reference(field_now, earlier, speed_square):
    for step in range(STEPS):
        later = march_step(jnp.pad(field_now, ((1, 1), (1, 1), (1, 1), (0, 0)), mode='constant'), earlier, speed_square)
        earlier, field_now = (field_now, later)
    line_mean = lax.optimization_barrier(jnp.mean(field_now, axis=2, keepdims=True))
    centred = field_now - line_mean
    line_variance = lax.optimization_barrier(jnp.mean(centred * centred, axis=2, keepdims=True))
    scaled_field = centred * lax.rsqrt(line_variance + 0.0001)
    return (scaled_field, field_now)
```

```python
import functools

import jax
import jax.numpy as jnp
from jax import lax
from jax.experimental import pallas as pl
from jax.experimental.pallas import tpu as pltpu
from jax.sharding import PartitionSpec as P

STEPS = 3
R = 4
PAD = 8
MESH = pl.DeviceIdType.MESH
F32 = jnp.float32


def march_kernel(
    shape, sizes, now_hbm, before_hbm, speed_hbm,
    last, mean_out, scale_out,
    even, odd, speed, stats,
    load_sem, z_send, z_recv, x_send, x_recv, y_send, y_recv, s_send, s_recv,
):
    J, I, K, M = shape
    rows, cols, slabs = sizes
    N = I // R
    LINES = J * R
    row, col, slab = (lax.axis_index(a) for a in ("rows", "cols", "slabs"))
    has = {
        "rows": (row > 0, row < rows - 1),
        "cols": (col > 0, col < cols - 1),
        "slabs": (slab > 0, slab < slabs - 1),
    }
    beside = {
        "rows": (row - 1, row + 1),
        "cols": (col - 1, col + 1),
        "slabs": (slab - 1, slab + 1),
    }
    jj, kk = pl.ds(1, J), pl.ds(PAD, K)
    fields = (even, odd, even)

    def span(c):
        return pl.ds(c * R, R)

    def inner(c):
        return pl.ds(1 + c * R, R)

    def z_copy(s, side, c):
        f = fields[s]
        edge = 0 if side == 0 else J - 1
        src = now_hbm.at[edge, span(c)] if s == 0 else f.at[1 + edge, inner(c), kk]
        dst = f.at[J + 1 if side == 0 else 0, inner(c), kk]
        return pltpu.make_async_remote_copy(
            src, dst, z_send.at[s, side, c], z_recv.at[s, side, c],
            device_id={"rows": beside["rows"][side]}, device_id_type=MESH)

    def x_copy(s, side):
        f = fields[s]
        edge = 0 if side == 0 else I - 1
        src = now_hbm.at[:, edge] if s == 0 else f.at[jj, 1 + edge, kk]
        dst = f.at[jj, I + 1 if side == 0 else 0, kk]
        return pltpu.make_async_remote_copy(
            src, dst, x_send.at[s, side], x_recv.at[s, side],
            device_id={"cols": beside["cols"][side]}, device_id_type=MESH)

    def y_copy(s, side, c):
        f = fields[s]
        edge = 0 if side == 0 else K - PAD
        if s == 0:
            src = now_hbm.at[:, span(c), pl.ds(edge, PAD)]
        else:
            src = f.at[jj, inner(c), pl.ds(PAD + edge, PAD)]
        dst = f.at[jj, inner(c), pl.ds(PAD + K if side == 0 else 0, PAD)]
        return pltpu.make_async_remote_copy(
            src, dst, y_send.at[s, side, c], y_recv.at[s, side, c],
            device_id={"slabs": beside["slabs"][side]}, device_id_type=MESH)

    def s_copy(d, c):
        part = stats.at[slab, c]
        return pltpu.make_async_remote_copy(
            part, part, s_send.at[d - 1, c], s_recv.at[d - 1, c],
            device_id={"slabs": lax.rem(slab + d, slabs)}, device_id_type=MESH)

    def load(k, c):
        src, dst = (
            (now_hbm, even.at[jj, inner(c), kk]),
            (before_hbm, odd.at[jj, inner(c), kk]),
            (speed_hbm, speed.at[:, span(c)]),
        )[k]
        return pltpu.make_async_copy(src.at[:, span(c)], dst, load_sem.at[k, c])

    barrier = pltpu.get_barrier_semaphore()
    count = jnp.int32(slabs - 1)
    for axis in ("rows", "cols"):
        for side in (0, 1):
            there = has[axis][side]
            count = count + there.astype(jnp.int32)

            @pl.when(there)
            def _():
                pl.semaphore_signal(barrier, inc=1, device_id={axis: beside[axis][side]}, device_id_type=MESH)
    for d in range(1, slabs):
        pl.semaphore_signal(barrier, inc=1, device_id={"slabs": lax.rem(slab + d, slabs)}, device_id_type=MESH)

    @pl.loop(0, N)
    def _(c):
        for k in range(3):
            load(k, c).start()

    for f in (even, odd):
        for side, (z, x, y) in enumerate(((0, 0, 0), (J + 1, I + 1, PAD + K))):
            @pl.when(jnp.logical_not(has["rows"][side]))
            def _():
                @pl.loop(0, I)
                def _(i):
                    f[z, 1 + i, kk] = jnp.zeros((K, M), F32)

            @pl.when(jnp.logical_not(has["cols"][side]))
            def _():
                @pl.loop(0, J)
                def _(j):
                    f[1 + j, x, kk] = jnp.zeros((K, M), F32)

            @pl.when(jnp.logical_not(has["slabs"][side]))
            def _():
                @pl.loop(0, I)
                def _(i):
                    for j in range(J):
                        f[1 + j, 1 + i, pl.ds(y, PAD)] = jnp.zeros((PAD, M), F32)

    pl.semaphore_wait(barrier, count)

    def for_sides(axis, act):
        for side in (0, 1):
            @pl.when(has[axis][side])
            def _():
                act(side)

    @pl.loop(0, N)
    def _(c):
        for_sides("rows", lambda side: z_copy(0, side, c).start())
        for_sides("slabs", lambda side: y_copy(0, side, c).start())

    for_sides("cols", lambda side: x_copy(0, side).start())

    def line(s, j, i):
        f, g = fields[s], fields[(s + 1) % 2]
        centre = f[1 + j, 1 + i, kk]
        total = f[j, 1 + i, kk] + f[j + 2, 1 + i, kk]
        total = total + (f[1 + j, i, kk] + f[1 + j, i + 2, kk])
        total = total + (f[1 + j, 1 + i, pl.ds(PAD - 1, K)] + f[1 + j, 1 + i, pl.ds(PAD + 1, K)])
        old = g[1 + j, 1 + i, kk]
        return (2.0 * centre - old) + speed[j, i] * (total - 6.0 * centre)

    def step_lines(s, c, planes):
        first, stride = planes

        @pl.loop(0, 2)
        def _(p):
            j = first + stride * p
            if s < STEPS - 1:
                @pl.loop(0, R)
                def _(r):
                    i = c * R + r
                    fields[(s + 1) % 2][1 + j, 1 + i, kk] = line(s, j, i)
            else:
                @pl.loop(0, R)
                def _(r):
                    i = c * R + r
                    value = line(s, j, i)
                    last[j, i] = value
                    mean = jnp.sum(value, axis=0, keepdims=True) * (1.0 / K)
                    away = value - mean
                    at = pl.ds(j * R + r, 1)
                    stats[slab, c, 0, at, :] = mean
                    stats[slab, c, 1, at, :] = jnp.sum(away * away, axis=0, keepdims=True)

    def finish(c):
        for d in range(1, slabs):
            s_copy(d, c).wait_recv()
        means = [stats[b, c, 0] for b in range(slabs)]
        mean = sum(means[1:], means[0]) * (1.0 / slabs)
        spread = sum((stats[b, c, 1] for b in range(1, slabs)), stats[0, c, 1])
        apart = sum(((m - mean) * (m - mean) for m in means[1:]), (means[0] - mean) * (means[0] - mean))
        variance = (spread + K * apart) * (1.0 / (K * slabs))
        mean_out[c] = mean
        scale_out[c] = lax.rsqrt(variance + 0.0001)

    def wait_sides(axis, copy):
        for side in (0, 1):
            @pl.when(has[axis][1 - side])
            def _():
                copy(side).wait_recv()

    for s in range(STEPS):
        if s == 0:
            load(0, 0).wait()

        @pl.loop(0, N)
        def _(c):
            if s == 0:
                @pl.when(c + 1 < N)
                def _():
                    load(0, c + 1).wait()

                for k in (1, 2):
                    load(k, c).wait()
            wait_sides("slabs", lambda side: y_copy(s, side, c))

            @pl.when(jnp.logical_and(c == 0, has["cols"][0]))
            def _():
                x_copy(s, 1).wait_recv()

            @pl.when(jnp.logical_and(c == N - 1, has["cols"][1]))
            def _():
                x_copy(s, 0).wait_recv()

            if s < STEPS - 1:
                wait_sides("rows", lambda side: z_copy(s, side, c))
                step_lines(s, c, (0, J - 1))
                step_lines(s, c, (1, 1))
                for_sides("rows", lambda side: z_copy(s + 1, side, c).start())
                for_sides("slabs", lambda side: y_copy(s + 1, side, c).start())

                @pl.when(jnp.logical_and(c == 0, has["cols"][0]))
                def _():
                    x_copy(s + 1, 0).start()

                @pl.when(jnp.logical_and(c == N - 1, has["cols"][1]))
                def _():
                    x_copy(s + 1, 1).start()
            else:
                step_lines(s, c, (1, 1))
                wait_sides("rows", lambda side: z_copy(s, side, c))
                step_lines(s, c, (0, J - 1))
                for d in range(1, slabs):
                    s_copy(d, c).start()

                @pl.when(c > 0)
                def _():
                    finish(c - 1)

    for s in range(STEPS):
        @pl.loop(0, N)
        def _(c):
            for_sides("rows", lambda side: z_copy(s, side, c).wait_send())
            for_sides("slabs", lambda side: y_copy(s, side, c).wait_send())

        for_sides("cols", lambda side: x_copy(s, side).wait_send())

    finish(N - 1)

    @pl.loop(0, N)
    def _(c):
        for d in range(1, slabs):
            s_copy(d, c).wait_send()


def write_kernel(shape, last, mean, scale, scaled_hbm, end_hbm, scaled, sems):
    J, I, K, M = shape
    N = I // R

    def end_copy(c):
        span = pl.ds(c * R, R)
        return pltpu.make_async_copy(last.at[:, span], end_hbm.at[:, span], sems.at[0, c])

    def scaled_copy(c):
        span = pl.ds(c * R, R)
        return pltpu.make_async_copy(scaled.at[:, span], scaled_hbm.at[:, span], sems.at[1, c])

    @pl.loop(0, N)
    def _(c):
        end_copy(c).start()

    @pl.loop(0, N)
    def _(c):
        @pl.loop(0, J)
        def _(j):
            for r in range(R):
                at = pl.ds(j * R + r, 1)
                i = c * R + r
                scaled[j, i] = (last[j, i] - mean[c, at, :]) * scale[c, at, :]
        scaled_copy(c).start()

    @pl.loop(0, N)
    def _(c):
        end_copy(c).wait()
        scaled_copy(c).wait()


def shards(sizes, field_now, earlier, speed_square):
    shape = field_now.shape
    J, I, K, M = shape
    N = I // R
    slabs = sizes[2]
    hbm = pl.BlockSpec(memory_space=pltpu.HBM)
    vmem = pl.BlockSpec(memory_space=pltpu.VMEM)
    dma = pltpu.SemaphoreType.DMA
    padded = pltpu.VMEM((J + 2, I + 2, K + 2 * PAD, M), F32)
    last, mean, scale = pl.pallas_call(
        functools.partial(march_kernel, shape, sizes),
        out_shape=(
            pltpu.VMEM(shape, F32),
            pltpu.VMEM((N, J * R, M), F32),
            pltpu.VMEM((N, J * R, M), F32),
        ),
        in_specs=[hbm, hbm, hbm],
        out_specs=(vmem, vmem, vmem),
        scratch_shapes=[
            padded,
            padded,
            pltpu.VMEM(shape, F32),
            pltpu.VMEM((slabs, N, 2, J * R, M), F32),
            dma((3, N)),
            dma((STEPS, 2, N)),
            dma((STEPS, 2, N)),
            dma((STEPS, 2)),
            dma((STEPS, 2)),
            dma((STEPS, 2, N)),
            dma((STEPS, 2, N)),
            dma((slabs - 1, N)),
            dma((slabs - 1, N)),
        ],
        compiler_params=pltpu.CompilerParams(
            collective_id=0, has_side_effects=True, vmem_limit_bytes=44 * 2**20
        ),
        name="march",
    )(field_now, earlier, speed_square)
    return pl.pallas_call(
        functools.partial(write_kernel, shape),
        out_shape=(jax.ShapeDtypeStruct(shape, F32), jax.ShapeDtypeStruct(shape, F32)),
        in_specs=[vmem, vmem, vmem],
        out_specs=(hbm, hbm),
        scratch_shapes=[pltpu.VMEM(shape, F32), dma((2, N))],
        compiler_params=pltpu.CompilerParams(vmem_limit_bytes=12 * 2**20),
        name="write",
    )(last, mean, scale)


def solution(mesh):
    placed = P("rows", "cols", "slabs", None)
    sizes = tuple(mesh.shape[a] for a in ("rows", "cols", "slabs"))
    return jax.shard_map(
        functools.partial(shards, sizes),
        mesh=mesh,
        in_specs=(placed, placed, placed),
        out_specs=(placed, placed),
        check_vma=False,
    )
```

```python
import functools

import jax
import jax.numpy as jnp
from jax import lax
from jax.experimental import pallas as pl
from jax.experimental.pallas import tpu as pltpu
from jax.sharding import PartitionSpec as P

STEPS = 3
PAD = 8
MESH = pl.DeviceIdType.MESH
F32 = jnp.float32


def chunks_of(rows, step):
    size = max(rows // 4, 2)
    cut = [(a, size) for a in range(0, rows, size)]
    if step == STEPS - 1:
        first, size = cut.pop()
        cut += [(first, size // 2), (first + size // 2, size // 2)]
    return cut


def march_kernel(
    shape, sizes, now_hbm, before_hbm, speed_hbm,
    last, lines_out,
    even, odd, speed, stats,
    load_sem, z_send, z_recv, x_send, x_recv, y_send, y_recv, s_send, s_recv,
    passed_on, further,
):
    J, I, K, M = shape
    rows, cols, slabs = sizes
    row, col, slab = (lax.axis_index(a) for a in ("rows", "cols", "slabs"))
    has = {
        "rows": (row > 0, row < rows - 1),
        "cols": (col > 0, col < cols - 1),
        "slabs": (slab > 0, slab < slabs - 1),
    }
    beside = {
        "rows": (row - 1, row + 1),
        "cols": (col - 1, col + 1),
        "slabs": (slab - 1, slab + 1),
    }
    upper_core = lax.rem(row, 2) == 1
    jj, ii, kk = pl.ds(1, J), pl.ds(1, I), pl.ds(PAD, K)
    fields = (even, odd, even)
    chunks = [chunks_of(I, s) for s in range(STEPS)]
    slot = [{cut: n for n, cut in enumerate(chunks[s])} for s in range(STEPS)]
    base = [(s % 2) * len(chunks[-1]) for s in range(STEPS)]

    def z_copy(s, side, cut):
        f = fields[s]
        a, n = cut
        edge = 0 if side == 0 else J - 1
        src = now_hbm.at[edge, pl.ds(a, n)] if s == 0 else f.at[1 + edge, pl.ds(1 + a, n), kk]
        dst = f.at[J + 1 if side == 0 else 0, pl.ds(1 + a, n), kk]
        return pltpu.make_async_remote_copy(
            src, dst, z_send.at[side], z_recv.at[side, base[s] + slot[s][cut]],
            device_id={"rows": beside["rows"][side]}, device_id_type=MESH)

    def x_copy(s, side):
        f = fields[s]
        edge = 0 if side == 0 else I - 1
        src = now_hbm.at[:, edge] if s == 0 else f.at[jj, 1 + edge, kk]
        dst = f.at[jj, I + 1 if side == 0 else 0, kk]
        return pltpu.make_async_remote_copy(
            src, dst, x_send.at[side], x_recv.at[s % 2, side],
            device_id={"cols": beside["cols"][side]}, device_id_type=MESH)

    def y_copy(s, side):
        f = fields[s]
        edge = 0 if side == 0 else K - 1
        src = now_hbm.at[:, :, pl.ds(edge, 1)] if s == 0 else f.at[jj, ii, pl.ds(PAD + edge, 1)]
        dst = f.at[jj, ii, pl.ds(PAD + K if side == 0 else PAD - 1, 1)]
        return pltpu.make_async_remote_copy(
            src, dst, y_send.at[side], y_recv.at[s % 2, side],
            device_id={"slabs": beside["slabs"][side]}, device_id_type=MESH)

    far = jnp.where(upper_core, J - 1, 0)
    early, late = 0, 1

    def s_copy(part, d, planes, cut):
        ref = stats.at[slab, :, planes, pl.ds(*cut)]
        return pltpu.make_async_remote_copy(
            ref, ref, s_send, s_recv.at[part, d - 1],
            device_id={"slabs": lax.rem(slab + d, slabs)}, device_id_type=MESH)

    def send_sums(part, planes, cut):
        for d in range(1, slabs):
            s_copy(part, d, planes, cut).start()

    def load(ref, buffer, c, sem):
        a, n = chunks[0][c]
        start = 1 if buffer is not speed else 0
        planes = jj if buffer is not speed else pl.ds(0, J)
        width = kk if buffer is not speed else pl.ds(0, K)
        return pltpu.make_async_copy(
            ref.at[:, pl.ds(a, n)], buffer.at[planes, pl.ds(start + a, n), width], load_sem.at[sem])

    def start_loads(c):
        if c + 1 < len(chunks[0]):
            load(now_hbm, even, c + 1, c + 1).start()
        if c < len(chunks[0]):
            load(before_hbm, odd, c, c + 1).start()
            load(speed_hbm, speed, c, c + 1).start()

    def wait_loads(c):
        a, n = chunks[0][c]
        amount = pl.ds(0, 3 * n if c + 1 < len(chunks[0]) else 2 * n)
        pltpu.make_async_copy(speed_hbm.at[:, amount], speed.at[:, amount], load_sem.at[c + 1]).wait()

    def for_sides(axis, act):
        for side in (0, 1):
            @pl.when(has[axis][side])
            def _():
                act(side)

    def wait_sides(axis, copy):
        for side in (0, 1):
            @pl.when(has[axis][1 - side])
            def _():
                copy(side).wait_recv()

    lower_core = jnp.logical_not(upper_core)
    around = [(axis, side) for axis in ("cols", "slabs") for side in (0, 1)]

    def number(places):
        return sum((has[axis][side].astype(jnp.int32) for axis, side in places), jnp.int32(0))

    def greet(sem, axis, side, when):
        @pl.when(jnp.logical_and(has[axis][side], when))
        def _():
            pl.semaphore_signal(sem, inc=1, device_id={axis: beside[axis][side]}, device_id_type=MESH)

    barrier = pltpu.get_barrier_semaphore()
    for side in (0, 1):
        greet(barrier, "rows", side, True)
    for axis, side in around:
        greet(barrier, axis, side, upper_core)
    load(now_hbm, even, 0, 0).start()
    start_loads(0)
    pl.semaphore_wait(barrier, number([("rows", 0), ("rows", 1)]) + jnp.where(upper_core, number(around), 0))
    for cut in chunks[0]:
        for_sides("rows", lambda side: z_copy(0, side, cut).start())
    for axis, side in around:
        greet(passed_on, axis, side, upper_core)
    pl.semaphore_wait(passed_on, jnp.where(upper_core, number(around), 1))

    @pl.when(upper_core)
    def _():
        pl.semaphore_signal(passed_on, inc=1, device_id={"rows": row - 1}, device_id_type=MESH)

    for_sides("slabs", lambda side: y_copy(0, side).start())
    for_sides("cols", lambda side: x_copy(0, side).start())
    start_loads(1)

    def tell(t):
        for side in (0, 1):
            greet(further.at[t], "slabs", side, True)

    def hear(t):
        pl.semaphore_wait(further.at[t], number([("slabs", 0), ("slabs", 1)]))

    tell(0)

    for f in (even, odd):
        for side, (z, x, y) in enumerate(((0, 0, PAD - 1), (J + 1, I + 1, PAD + K))):
            @pl.when(jnp.logical_not(has["rows"][side]))
            def _():
                @pl.loop(0, I)
                def _(i):
                    f[z, 1 + i, kk] = jnp.zeros((K, M), F32)

            @pl.when(jnp.logical_not(has["cols"][side]))
            def _():
                @pl.loop(0, J)
                def _(j):
                    f[1 + j, x, kk] = jnp.zeros((K, M), F32)

            @pl.when(jnp.logical_not(has["slabs"][side]))
            def _():
                @pl.loop(0, I)
                def _(i):
                    for j in range(J):
                        f[1 + j, 1 + i, pl.ds(y, 1)] = jnp.zeros((1, M), F32)

    def line(s, j, i):
        f, g = fields[s], fields[(s + 1) % 2]
        centre = f[1 + j, 1 + i, kk]
        total = f[j, 1 + i, kk] + f[j + 2, 1 + i, kk]
        total = total + (f[1 + j, i, kk] + f[1 + j, i + 2, kk])
        total = total + (f[1 + j, 1 + i, pl.ds(PAD - 1, K)] + f[1 + j, 1 + i, pl.ds(PAD + 1, K)])
        old = g[1 + j, 1 + i, kk]
        return (2.0 * centre - old) + speed[j, i] * (total - 6.0 * centre)

    def step_plane(s, cut, j):
        a, n = cut

        @pl.loop(a, a + n)
        def _(i):
            value = line(s, j, i)
            if s < STEPS - 1:
                fields[(s + 1) % 2][1 + j, 1 + i, kk] = value
            else:
                last[j, i] = value
                mean = jnp.sum(value, axis=0, keepdims=True) * (1.0 / K)
                away = value - mean
                stats[slab, 0, j, pl.ds(i, 1)] = mean
                stats[slab, 1, j, pl.ds(i, 1)] = jnp.sum(away * away, axis=0, keepdims=True)

    def step_inside(s, cut):
        @pl.loop(1, J - 1)
        def _(j):
            step_plane(s, cut, j)

    def wait_below(s, cut, when):
        @pl.when(jnp.logical_and(has["rows"][0], when))
        def _():
            z_copy(s, 1, cut).wait_recv()

    def wait_above(s, cut, when):
        @pl.when(jnp.logical_and(has["rows"][1], when))
        def _():
            z_copy(s, 0, cut).wait_recv()

    def step_outside(s, cut, between=None):
        wait_below(s, cut, upper_core)
        wait_above(s, cut, lower_core)
        step_plane(s, cut, J - 1 - far)
        if between is not None:
            between()
        wait_below(s, cut, lower_core)
        wait_above(s, cut, upper_core)
        step_plane(s, cut, far)

    def finish(planes, rows_i):
        @pl.loop(*planes)
        def _(j):
            at = pl.ds(*rows_i)
            means = [stats[b, 0, j, at] for b in range(slabs)]
            mean = sum(means[1:], means[0]) * (1.0 / slabs)
            spread = sum((stats[b, 1, j, at] for b in range(1, slabs)), stats[0, 1, j, at])
            apart = sum(((m - mean) * (m - mean) for m in means[1:]), (means[0] - mean) * (means[0] - mean))
            variance = (spread + K * apart) * (1.0 / (K * slabs))
            lines_out[0, j, at] = mean
            lines_out[1, j, at] = lax.rsqrt(variance + 0.0001)

    load(now_hbm, even, 0, 0).wait()
    for s in range(STEPS):
        for c, cut in enumerate(chunks[s]):
            a, n = cut
            if s == 0:
                start_loads(c + 2)
                wait_loads(c)
            if c == 0:
                wait_sides("slabs", lambda side: y_copy(s, side))

                @pl.when(has["cols"][0])
                def _():
                    x_copy(s, 1).wait_recv()
            if a + n == I:
                @pl.when(has["cols"][1])
                def _():
                    x_copy(s, 0).wait_recv()
            if s == 1 and c < slabs - 2:
                hear(c)
                if c + 1 < slabs - 2:
                    tell(c + 1)
            if s < STEPS - 1:
                step_outside(s, cut)
                for later in chunks[s + 1]:
                    if a <= later[0] < a + n:
                        for_sides("rows", lambda side: z_copy(s + 1, side, later).start())
                step_inside(s, cut)
                if c == 0:
                    @pl.when(has["cols"][0])
                    def _():
                        x_copy(s + 1, 0).start()
                if a + n == I:
                    @pl.when(has["cols"][1])
                    def _():
                        x_copy(s + 1, 1).start()

                    for_sides("slabs", lambda side: y_copy(s + 1, side).start())
            else:
                step_inside(s, cut)
                if cut != chunks[s][-1]:
                    step_outside(s, cut)
                    send_sums(early, pl.ds(0, J), cut)
                else:
                    nearer = pl.ds(jnp.where(upper_core, 0, 1), J - 1)
                    step_outside(s, cut, lambda: send_sums(early, nearer, cut))
                    send_sums(late, pl.ds(far, 1), cut)

    tail = chunks[-1][-1]
    eight = pl.ds(0, 8)
    soon = even.at[0, pl.ds(0, 2 * (J * I - tail[1]) // 8), eight]
    for d in range(1, slabs):
        pltpu.make_async_remote_copy(
            soon, soon, s_send, s_recv.at[early, d - 1],
            device_id={"slabs": lax.rem(slab + d, slabs)}, device_id_type=MESH).wait_recv()
    finish((0, J), (0, tail[0]))
    finish((jnp.where(upper_core, 0, 1), jnp.where(upper_core, J - 1, J)), tail)
    for d in range(1, slabs):
        s_copy(late, d, pl.ds(far, 1), tail).wait_recv()
    finish((far, far + 1), tail)

    def all_left(ref, send, axis, side):
        pltpu.make_async_remote_copy(
            ref, ref, send, s_recv.at[0, 0],
            device_id={axis: beside[axis][side]}, device_id_type=MESH).wait_send()

    for_sides("rows", lambda side: all_left(speed.at[pl.ds(0, STEPS)], z_send.at[side], "rows", side))
    for_sides("cols", lambda side: all_left(speed.at[:, pl.ds(0, STEPS)], x_send.at[side], "cols", side))
    for_sides("slabs", lambda side: all_left(speed.at[:, :, pl.ds(0, STEPS)], y_send.at[side], "slabs", side))
    pltpu.make_async_remote_copy(
        stats.at[pl.ds(0, slabs - 1)], stats.at[pl.ds(0, slabs - 1)], s_send, s_recv.at[0, 0],
        device_id={"slabs": lax.rem(slab + 1, slabs)}, device_id_type=MESH).wait_send()


def write_kernel(shape, pieces, last, lines, scaled_hbm, end_hbm, scaled, sems):
    J, I, K, M = shape
    n = I // pieces

    @pl.loop(0, pieces)
    def _(c):
        span = pl.ds(c * n, n)
        pltpu.make_async_copy(last.at[:, span], end_hbm.at[:, span], sems.at[0]).start()

    @pl.loop(0, pieces)
    def _(c):
        @pl.loop(0, n)
        def _(r):
            i = c * n + r
            for j in range(J):
                at = pl.ds(i, 1)
                scaled[j, i] = (last[j, i] - lines[0, j, at]) * lines[1, j, at]

        span = pl.ds(c * n, n)
        pltpu.make_async_copy(scaled.at[:, span], scaled_hbm.at[:, span], sems.at[1]).start()

    pltpu.make_async_copy(last, end_hbm, sems.at[0]).wait()
    pltpu.make_async_copy(scaled, scaled_hbm, sems.at[1]).wait()


def shards(sizes, field_now, earlier, speed_square):
    shape = field_now.shape
    J, I, K, M = shape
    slabs = sizes[2]
    hbm = pl.BlockSpec(memory_space=pltpu.HBM)
    vmem = pl.BlockSpec(memory_space=pltpu.VMEM)
    dma = pltpu.SemaphoreType.DMA
    padded = pltpu.VMEM((J + 2, I + 2, K + 2 * PAD, M), F32)
    arrivals = len(chunks_of(I, 1)) + len(chunks_of(I, STEPS - 1))
    last, lines = pl.pallas_call(
        functools.partial(march_kernel, shape, sizes),
        out_shape=(pltpu.VMEM(shape, F32), pltpu.VMEM((2, J, I, M), F32)),
        in_specs=[hbm, hbm, hbm],
        out_specs=(vmem, vmem),
        scratch_shapes=[
            padded,
            padded,
            pltpu.VMEM(shape, F32),
            pltpu.VMEM((slabs, 2, J, I, M), F32),
            dma((1 + len(chunks_of(I, 0)),)),
            dma((2,)),
            dma((2, arrivals)),
            dma((2,)),
            dma((2, 2)),
            dma((2,)),
            dma((2, 2)),
            dma,
            dma((2, slabs - 1)),
            pltpu.SemaphoreType.REGULAR,
            pltpu.SemaphoreType.REGULAR((slabs - 2,)),
        ],
        compiler_params=pltpu.CompilerParams(
            collective_id=0, has_side_effects=True, vmem_limit_bytes=44 * 2**20
        ),
        name="march",
    )(field_now, earlier, speed_square)
    return pl.pallas_call(
        functools.partial(write_kernel, shape, 8),
        out_shape=(jax.ShapeDtypeStruct(shape, F32), jax.ShapeDtypeStruct(shape, F32)),
        in_specs=[vmem, vmem],
        out_specs=(hbm, hbm),
        scratch_shapes=[pltpu.VMEM(shape, F32), dma((2,))],
        compiler_params=pltpu.CompilerParams(vmem_limit_bytes=12 * 2**20),
        name="write",
    )(last, lines)


def solution(mesh):
    placed = P("rows", "cols", "slabs", None)
    sizes = tuple(mesh.shape[a] for a in ("rows", "cols", "slabs"))
    return jax.shard_map(
        functools.partial(shards, sizes),
        mesh=mesh,
        in_specs=(placed, placed, placed),
        out_specs=(placed, placed),
        check_vma=False,
    )
```

```python
import functools

import jax
import jax.numpy as jnp
from jax import lax
from jax.experimental import pallas as pl
from jax.experimental.pallas import tpu as pltpu
from jax.sharding import PartitionSpec as P

STEPS = 3
PAD = 8
MESH = pl.DeviceIdType.MESH
F32 = jnp.float32


def chunks_of(rows, step):
    half = rows // 2
    cut = [(0, half), (half, half)]
    if step == STEPS - 1:
        cut = [(0, half), (half, half // 2), (half + half // 2, half // 4), (half + 3 * half // 4, half // 4)]
    return cut


def march_kernel(
    shape, sizes, now_hbm, before_hbm, speed_hbm,
    last, lines_out,
    even, odd, speed, stats,
    load_sem, z_send, z_recv, x_send, x_recv, y_send, y_recv, s_send, s_recv,
    passed_on, further,
):
    J, I, K, M = shape
    rows, cols, slabs = sizes
    row, col, slab = (lax.axis_index(a) for a in ("rows", "cols", "slabs"))
    has = {
        "rows": (row > 0, row < rows - 1),
        "cols": (col > 0, col < cols - 1),
        "slabs": (slab > 0, slab < slabs - 1),
    }
    beside = {
        "rows": (row - 1, row + 1),
        "cols": (col - 1, col + 1),
        "slabs": (slab - 1, slab + 1),
    }
    upper_core = lax.rem(row, 2) == 1
    jj, ii, kk = pl.ds(1, J), pl.ds(1, I), pl.ds(PAD, K)
    fields = (even, odd, even)
    chunks = [chunks_of(I, s) for s in range(STEPS)]
    slot = [{cut: n for n, cut in enumerate(chunks[s])} for s in range(STEPS)]
    base = [(s % 2) * len(chunks[-1]) for s in range(STEPS)]

    def z_copy(s, side, cut):
        f = fields[s]
        a, n = cut
        edge = 0 if side == 0 else J - 1
        src = now_hbm.at[edge, pl.ds(a, n)] if s == 0 else f.at[1 + edge, pl.ds(1 + a, n), kk]
        dst = f.at[J + 1 if side == 0 else 0, pl.ds(1 + a, n), kk]
        return pltpu.make_async_remote_copy(
            src, dst, z_send.at[side], z_recv.at[side, base[s] + slot[s][cut]],
            device_id={"rows": beside["rows"][side]}, device_id_type=MESH)

    def x_copy(s, side):
        f = fields[s]
        edge = 0 if side == 0 else I - 1
        src = now_hbm.at[:, edge] if s == 0 else f.at[jj, 1 + edge, kk]
        dst = f.at[jj, I + 1 if side == 0 else 0, kk]
        return pltpu.make_async_remote_copy(
            src, dst, x_send.at[side], x_recv.at[s % 2, side],
            device_id={"cols": beside["cols"][side]}, device_id_type=MESH)

    def y_copy(s, side):
        f = fields[s]
        edge = 0 if side == 0 else K - 1
        src = now_hbm.at[:, :, pl.ds(edge, 1)] if s == 0 else f.at[jj, ii, pl.ds(PAD + edge, 1)]
        dst = f.at[jj, ii, pl.ds(PAD + K if side == 0 else PAD - 1, 1)]
        return pltpu.make_async_remote_copy(
            src, dst, y_send.at[side], y_recv.at[s % 2, side],
            device_id={"slabs": beside["slabs"][side]}, device_id_type=MESH)

    far = jnp.where(upper_core, J - 1, 0)
    early, late = 0, 1

    def s_copy(part, d, planes, cut):
        ref = stats.at[slab, :, planes, pl.ds(*cut)]
        return pltpu.make_async_remote_copy(
            ref, ref, s_send, s_recv.at[part, d - 1],
            device_id={"slabs": lax.rem(slab + d, slabs)}, device_id_type=MESH)

    def send_sums(part, planes, cut):
        for d in range(1, slabs):
            s_copy(part, d, planes, cut).start()

    def load(ref, buffer, c, sem):
        a, n = chunks[0][c]
        start = 1 if buffer is not speed else 0
        planes = jj if buffer is not speed else pl.ds(0, J)
        width = kk if buffer is not speed else pl.ds(0, K)
        return pltpu.make_async_copy(
            ref.at[:, pl.ds(a, n)], buffer.at[planes, pl.ds(start + a, n), width], load_sem.at[sem])

    count = len(chunks[0])

    def start_loads(c):
        if c + 1 < count:
            load(now_hbm, even, c + 1, c + 1).start()
        if c < count:
            load(before_hbm, odd, c, count + c).start()
            load(speed_hbm, speed, c, count + c).start()

    def wait_loads(c):
        if c + 1 < count:
            load(now_hbm, even, c + 1, c + 1).wait()
        amount = pl.ds(0, 2 * chunks[0][c][1])
        pltpu.make_async_copy(speed_hbm.at[:, amount], speed.at[:, amount], load_sem.at[count + c]).wait()

    def for_sides(axis, act):
        for side in (0, 1):
            @pl.when(has[axis][side])
            def _():
                act(side)

    def wait_sides(axis, copy):
        for side in (0, 1):
            @pl.when(has[axis][1 - side])
            def _():
                copy(side).wait_recv()

    lower_core = jnp.logical_not(upper_core)
    around = [(axis, side) for axis in ("cols", "slabs") for side in (0, 1)]

    def number(places):
        return sum((has[axis][side].astype(jnp.int32) for axis, side in places), jnp.int32(0))

    def greet(sem, axis, side, when):
        @pl.when(jnp.logical_and(has[axis][side], when))
        def _():
            pl.semaphore_signal(sem, inc=1, device_id={axis: beside[axis][side]}, device_id_type=MESH)

    barrier = pltpu.get_barrier_semaphore()
    for side in (0, 1):
        greet(barrier, "rows", side, True)
    for axis, side in around:
        greet(barrier, axis, side, upper_core)
    load(now_hbm, even, 0, 0).start()
    start_loads(0)
    pl.semaphore_wait(barrier, number([("rows", 0), ("rows", 1)]) + jnp.where(upper_core, number(around), 0))
    for cut in chunks[0]:
        for_sides("rows", lambda side: z_copy(0, side, cut).start())
    for axis, side in around:
        greet(passed_on, axis, side, upper_core)
    pl.semaphore_wait(passed_on, jnp.where(upper_core, number(around), 1))

    @pl.when(upper_core)
    def _():
        pl.semaphore_signal(passed_on, inc=1, device_id={"rows": row - 1}, device_id_type=MESH)

    for_sides("slabs", lambda side: y_copy(0, side).start())
    for_sides("cols", lambda side: x_copy(0, side).start())
    start_loads(1)

    def tell(t):
        for side in (0, 1):
            greet(further.at[t], "slabs", side, True)

    def hear(t):
        pl.semaphore_wait(further.at[t], number([("slabs", 0), ("slabs", 1)]))

    tell(0)

    for f in (even, odd):
        for side, (z, x, y) in enumerate(((0, 0, PAD - 1), (J + 1, I + 1, PAD + K))):
            @pl.when(jnp.logical_not(has["rows"][side]))
            def _():
                @pl.loop(0, I)
                def _(i):
                    f[z, 1 + i, kk] = jnp.zeros((K, M), F32)

            @pl.when(jnp.logical_not(has["cols"][side]))
            def _():
                @pl.loop(0, J)
                def _(j):
                    f[1 + j, x, kk] = jnp.zeros((K, M), F32)

            @pl.when(jnp.logical_not(has["slabs"][side]))
            def _():
                @pl.loop(0, I)
                def _(i):
                    for j in range(J):
                        f[1 + j, 1 + i, pl.ds(y, 1)] = jnp.zeros((1, M), F32)

    def line(s, j, i):
        f, g = fields[s], fields[(s + 1) % 2]
        centre = f[1 + j, 1 + i, kk]
        total = f[j, 1 + i, kk] + f[j + 2, 1 + i, kk]
        total = total + (f[1 + j, i, kk] + f[1 + j, i + 2, kk])
        total = total + (f[1 + j, 1 + i, pl.ds(PAD - 1, K)] + f[1 + j, 1 + i, pl.ds(PAD + 1, K)])
        old = g[1 + j, 1 + i, kk]
        return (2.0 * centre - old) + speed[j, i] * (total - 6.0 * centre)

    def step_plane(s, cut, j):
        a, n = cut

        @pl.loop(a, a + n, unroll=4 if s == STEPS - 1 else None)
        def _(i):
            value = line(s, j, i)
            if s < STEPS - 1:
                fields[(s + 1) % 2][1 + j, 1 + i, kk] = value
            else:
                last[j, i] = value
                mean = jnp.sum(value, axis=0, keepdims=True) * (1.0 / K)
                away = value - mean
                stats[slab, 0, j, pl.ds(i, 1)] = mean
                stats[slab, 1, j, pl.ds(i, 1)] = jnp.sum(away * away, axis=0, keepdims=True)

    def step_inside(s, cut):
        @pl.loop(1, J - 1)
        def _(j):
            step_plane(s, cut, j)

    def wait_below(s, cut, when):
        @pl.when(jnp.logical_and(has["rows"][0], when))
        def _():
            z_copy(s, 1, cut).wait_recv()

    def wait_above(s, cut, when):
        @pl.when(jnp.logical_and(has["rows"][1], when))
        def _():
            z_copy(s, 0, cut).wait_recv()

    def step_outside(s, cut, between=None):
        wait_below(s, cut, upper_core)
        wait_above(s, cut, lower_core)
        step_plane(s, cut, J - 1 - far)
        if between is not None:
            between()
        wait_below(s, cut, lower_core)
        wait_above(s, cut, upper_core)
        step_plane(s, cut, far)

    def finish(planes, rows_i):
        @pl.loop(*planes)
        def _(j):
            at = pl.ds(*rows_i)
            means = [stats[b, 0, j, at] for b in range(slabs)]
            mean = sum(means[1:], means[0]) * (1.0 / slabs)
            spread = sum((stats[b, 1, j, at] for b in range(1, slabs)), stats[0, 1, j, at])
            apart = sum(((m - mean) * (m - mean) for m in means[1:]), (means[0] - mean) * (means[0] - mean))
            variance = (spread + K * apart) * (1.0 / (K * slabs))
            lines_out[0, j, at] = mean
            lines_out[1, j, at] = lax.rsqrt(variance + 0.0001)

    load(now_hbm, even, 0, 0).wait()
    for s in range(STEPS):
        for c, cut in enumerate(chunks[s]):
            a, n = cut
            if s == 0:
                start_loads(c + 2)
                wait_loads(c)
            if c == 0:
                wait_sides("slabs", lambda side: y_copy(s, side))

                @pl.when(has["cols"][0])
                def _():
                    x_copy(s, 1).wait_recv()
            if a + n == I:
                @pl.when(has["cols"][1])
                def _():
                    x_copy(s, 0).wait_recv()
            if s == 1 and c < slabs - 2:
                hear(c)
                if c + 1 < slabs - 2:
                    tell(c + 1)
            if s < STEPS - 1:
                step_outside(s, cut)
                step_inside(s, cut)
                for later in chunks[s + 1]:
                    if a <= later[0] < a + n:
                        for_sides("rows", lambda side: z_copy(s + 1, side, later).start())
                if c == 0:
                    @pl.when(has["cols"][0])
                    def _():
                        x_copy(s + 1, 0).start()
                if a + n == I:
                    @pl.when(has["cols"][1])
                    def _():
                        x_copy(s + 1, 1).start()

                    for_sides("slabs", lambda side: y_copy(s + 1, side).start())
            else:
                step_inside(s, cut)
                if cut != chunks[s][-1]:
                    step_outside(s, cut)
                    send_sums(early, pl.ds(0, J), cut)
                else:
                    nearer = pl.ds(jnp.where(upper_core, 0, 1), J - 1)
                    step_outside(s, cut, lambda: send_sums(early, nearer, cut))
                    send_sums(late, pl.ds(far, 1), cut)

    tail = chunks[-1][-1]
    eight = pl.ds(0, 8)
    soon = even.at[0, pl.ds(0, 2 * (J * I - tail[1]) // 8), eight]
    for d in range(1, slabs):
        pltpu.make_async_remote_copy(
            soon, soon, s_send, s_recv.at[early, d - 1],
            device_id={"slabs": lax.rem(slab + d, slabs)}, device_id_type=MESH).wait_recv()
    finish((0, J), (0, tail[0]))
    finish((jnp.where(upper_core, 0, 1), jnp.where(upper_core, J - 1, J)), tail)
    for d in range(1, slabs):
        s_copy(late, d, pl.ds(far, 1), tail).wait_recv()
    finish((far, far + 1), tail)

    def all_left(ref, send, axis, side):
        pltpu.make_async_remote_copy(
            ref, ref, send, s_recv.at[0, 0],
            device_id={axis: beside[axis][side]}, device_id_type=MESH).wait_send()

    for_sides("rows", lambda side: all_left(speed.at[pl.ds(0, STEPS)], z_send.at[side], "rows", side))
    for_sides("cols", lambda side: all_left(speed.at[:, pl.ds(0, STEPS)], x_send.at[side], "cols", side))
    for_sides("slabs", lambda side: all_left(speed.at[:, :, pl.ds(0, STEPS)], y_send.at[side], "slabs", side))
    pltpu.make_async_remote_copy(
        stats.at[pl.ds(0, slabs - 1)], stats.at[pl.ds(0, slabs - 1)], s_send, s_recv.at[0, 0],
        device_id={"slabs": lax.rem(slab + 1, slabs)}, device_id_type=MESH).wait_send()


def write_kernel(shape, pieces, last, lines, scaled_hbm, end_hbm, scaled, sems):
    J, I, K, M = shape
    n = I // pieces

    @pl.loop(0, pieces)
    def _(c):
        span = pl.ds(c * n, n)
        pltpu.make_async_copy(last.at[:, span], end_hbm.at[:, span], sems.at[0]).start()

    @pl.loop(0, pieces)
    def _(c):
        @pl.loop(0, n)
        def _(r):
            i = c * n + r
            for j in range(J):
                at = pl.ds(i, 1)
                scaled[j, i] = (last[j, i] - lines[0, j, at]) * lines[1, j, at]

        span = pl.ds(c * n, n)
        pltpu.make_async_copy(scaled.at[:, span], scaled_hbm.at[:, span], sems.at[1]).start()

    pltpu.make_async_copy(last, end_hbm, sems.at[0]).wait()
    pltpu.make_async_copy(scaled, scaled_hbm, sems.at[1]).wait()


def shards(sizes, field_now, earlier, speed_square):
    shape = field_now.shape
    J, I, K, M = shape
    slabs = sizes[2]
    hbm = pl.BlockSpec(memory_space=pltpu.HBM)
    vmem = pl.BlockSpec(memory_space=pltpu.VMEM)
    dma = pltpu.SemaphoreType.DMA
    padded = pltpu.VMEM((J + 2, I + 2, K + 2 * PAD, M), F32)
    arrivals = len(chunks_of(I, 1)) + len(chunks_of(I, STEPS - 1))
    last, lines = pl.pallas_call(
        functools.partial(march_kernel, shape, sizes),
        out_shape=(pltpu.VMEM(shape, F32), pltpu.VMEM((2, J, I, M), F32)),
        in_specs=[hbm, hbm, hbm],
        out_specs=(vmem, vmem),
        scratch_shapes=[
            padded,
            padded,
            pltpu.VMEM(shape, F32),
            pltpu.VMEM((slabs, 2, J, I, M), F32),
            dma((2 * len(chunks_of(I, 0)),)),
            dma((2,)),
            dma((2, arrivals)),
            dma((2,)),
            dma((2, 2)),
            dma((2,)),
            dma((2, 2)),
            dma,
            dma((2, slabs - 1)),
            pltpu.SemaphoreType.REGULAR,
            pltpu.SemaphoreType.REGULAR((slabs - 2,)),
        ],
        compiler_params=pltpu.CompilerParams(
            collective_id=0, has_side_effects=True, vmem_limit_bytes=44 * 2**20
        ),
        name="march",
    )(field_now, earlier, speed_square)
    return pl.pallas_call(
        functools.partial(write_kernel, shape, 16),
        out_shape=(jax.ShapeDtypeStruct(shape, F32), jax.ShapeDtypeStruct(shape, F32)),
        in_specs=[vmem, vmem],
        out_specs=(hbm, hbm),
        scratch_shapes=[pltpu.VMEM(shape, F32), dma((2,))],
        compiler_params=pltpu.CompilerParams(vmem_limit_bytes=12 * 2**20),
        name="write",
    )(last, lines)


def solution(mesh):
    placed = P("rows", "cols", "slabs", None)
    sizes = tuple(mesh.shape[a] for a in ("rows", "cols", "slabs"))
    return jax.shard_map(
        functools.partial(shards, sizes),
        mesh=mesh,
        in_specs=(placed, placed, placed),
        out_specs=(placed, placed),
        check_vma=False,
    )
```

```python
import functools

import jax
import jax.numpy as jnp
from jax import lax
from jax.experimental import pallas as pl
from jax.experimental.pallas import tpu as pltpu
from jax.sharding import PartitionSpec as P

STEPS = 3
PAD = 8
MESH = pl.DeviceIdType.MESH
F32 = jnp.float32


def chunks_of(rows, step):
    half = rows // 2
    cut = [(0, half), (half, half)]
    if step == STEPS - 1:
        cut = [(0, half), (half, half // 2), (half + half // 2, half // 4), (half + 3 * half // 4, half // 4)]
    return cut


def march_kernel(
    shape, sizes, now_hbm, before_hbm, speed_hbm,
    last, lines_out,
    even, odd, speed, stats,
    load_sem, z_send, z_recv, x_send, x_recv, y_send, y_recv, s_send, s_recv,
    passed_on, further,
):
    J, I, K, M = shape
    rows, cols, slabs = sizes
    row, col, slab = (lax.axis_index(a) for a in ("rows", "cols", "slabs"))
    has = {
        "rows": (row > 0, row < rows - 1),
        "cols": (col > 0, col < cols - 1),
        "slabs": (slab > 0, slab < slabs - 1),
    }
    beside = {
        "rows": (row - 1, row + 1),
        "cols": (col - 1, col + 1),
        "slabs": (slab - 1, slab + 1),
    }
    upper_core = lax.rem(row, 2) == 1
    jj, ii, kk = pl.ds(1, J), pl.ds(1, I), pl.ds(PAD, K)
    fields = (even, odd, even)
    chunks = [chunks_of(I, s) for s in range(STEPS)]
    slot = [{cut: n for n, cut in enumerate(chunks[s])} for s in range(STEPS)]
    base = [(s % 2) * len(chunks[-1]) for s in range(STEPS)]

    def z_copy(s, side, cut):
        f = fields[s]
        a, n = cut
        edge = 0 if side == 0 else J - 1
        src = now_hbm.at[edge, pl.ds(a, n)] if s == 0 else f.at[1 + edge, pl.ds(1 + a, n), kk]
        dst = f.at[J + 1 if side == 0 else 0, pl.ds(1 + a, n), kk]
        return pltpu.make_async_remote_copy(
            src, dst, z_send.at[side], z_recv.at[side, base[s] + slot[s][cut]],
            device_id={"rows": beside["rows"][side]}, device_id_type=MESH)

    def x_copy(s, side):
        f = fields[s]
        edge = 0 if side == 0 else I - 1
        src = now_hbm.at[:, edge] if s == 0 else f.at[jj, 1 + edge, kk]
        dst = f.at[jj, I + 1 if side == 0 else 0, kk]
        return pltpu.make_async_remote_copy(
            src, dst, x_send.at[side], x_recv.at[s % 2, side],
            device_id={"cols": beside["cols"][side]}, device_id_type=MESH)

    def y_copy(s, side):
        f = fields[s]
        edge = 0 if side == 0 else K - 1
        src = now_hbm.at[:, :, pl.ds(edge, 1)] if s == 0 else f.at[jj, ii, pl.ds(PAD + edge, 1)]
        dst = f.at[jj, ii, pl.ds(PAD + K if side == 0 else PAD - 1, 1)]
        return pltpu.make_async_remote_copy(
            src, dst, y_send.at[side], y_recv.at[s % 2, side],
            device_id={"slabs": beside["slabs"][side]}, device_id_type=MESH)

    far = jnp.where(upper_core, J - 1, 0)
    early, late = 0, 1

    def s_copy(part, d, planes, cut):
        ref = stats.at[slab, :, planes, pl.ds(*cut)]
        return pltpu.make_async_remote_copy(
            ref, ref, s_send, s_recv.at[part, d - 1],
            device_id={"slabs": lax.rem(slab + d, slabs)}, device_id_type=MESH)

    def send_sums(part, planes, cut):
        for d in range(1, slabs):
            s_copy(part, d, planes, cut).start()

    def load(ref, buffer, c, sem):
        a, n = chunks[0][c]
        start = 1 if buffer is not speed else 0
        planes = jj if buffer is not speed else pl.ds(0, J)
        width = kk if buffer is not speed else pl.ds(0, K)
        return pltpu.make_async_copy(
            ref.at[:, pl.ds(a, n)], buffer.at[planes, pl.ds(start + a, n), width], load_sem.at[sem])

    count = len(chunks[0])

    def start_loads(c):
        if c + 1 < count:
            load(now_hbm, even, c + 1, c + 1).start()
        if c < count:
            load(before_hbm, odd, c, count + c).start()
            load(speed_hbm, speed, c, count + c).start()

    def wait_loads(c):
        if c + 1 < count:
            load(now_hbm, even, c + 1, c + 1).wait()
        amount = pl.ds(0, 2 * chunks[0][c][1])
        pltpu.make_async_copy(speed_hbm.at[:, amount], speed.at[:, amount], load_sem.at[count + c]).wait()

    def for_sides(axis, act):
        for side in (0, 1):
            @pl.when(has[axis][side])
            def _():
                act(side)

    def wait_sides(axis, copy):
        for side in (0, 1):
            @pl.when(has[axis][1 - side])
            def _():
                copy(side).wait_recv()

    lower_core = jnp.logical_not(upper_core)
    around = [(axis, side) for axis in ("cols", "slabs") for side in (0, 1)]

    def number(places):
        return sum((has[axis][side].astype(jnp.int32) for axis, side in places), jnp.int32(0))

    def greet(sem, axis, side, when):
        @pl.when(jnp.logical_and(has[axis][side], when))
        def _():
            pl.semaphore_signal(sem, inc=1, device_id={axis: beside[axis][side]}, device_id_type=MESH)

    barrier = pltpu.get_barrier_semaphore()
    for side in (0, 1):
        greet(barrier, "rows", side, True)
    for axis, side in around:
        greet(barrier, axis, side, upper_core)
    load(now_hbm, even, 0, 0).start()
    start_loads(0)
    pl.semaphore_wait(barrier, number([("rows", 0), ("rows", 1)]) + jnp.where(upper_core, number(around), 0))
    for cut in chunks[0]:
        for_sides("rows", lambda side: z_copy(0, side, cut).start())
    for axis, side in around:
        greet(passed_on, axis, side, upper_core)
    pl.semaphore_wait(passed_on, jnp.where(upper_core, number(around), 1))

    @pl.when(upper_core)
    def _():
        pl.semaphore_signal(passed_on, inc=1, device_id={"rows": row - 1}, device_id_type=MESH)

    for_sides("slabs", lambda side: y_copy(0, side).start())
    for_sides("cols", lambda side: x_copy(0, side).start())
    start_loads(1)

    def tell(t):
        for side in (0, 1):
            greet(further.at[t], "slabs", side, True)

    def hear(t):
        pl.semaphore_wait(further.at[t], number([("slabs", 0), ("slabs", 1)]))

    tell(0)

    for f in (even, odd):
        for side, (z, x, y) in enumerate(((0, 0, PAD - 1), (J + 1, I + 1, PAD + K))):
            @pl.when(jnp.logical_not(has["rows"][side]))
            def _():
                @pl.loop(0, I)
                def _(i):
                    f[z, 1 + i, kk] = jnp.zeros((K, M), F32)

            @pl.when(jnp.logical_not(has["cols"][side]))
            def _():
                @pl.loop(0, J)
                def _(j):
                    f[1 + j, x, kk] = jnp.zeros((K, M), F32)

            @pl.when(jnp.logical_not(has["slabs"][side]))
            def _():
                @pl.loop(0, I)
                def _(i):
                    for j in range(J):
                        f[1 + j, 1 + i, pl.ds(y, 1)] = jnp.zeros((1, M), F32)

    def line(s, j, i):
        f, g = fields[s], fields[(s + 1) % 2]
        centre = f[1 + j, 1 + i, kk]
        total = f[j, 1 + i, kk] + f[j + 2, 1 + i, kk]
        total = total + (f[1 + j, i, kk] + f[1 + j, i + 2, kk])
        total = total + (f[1 + j, 1 + i, pl.ds(PAD - 1, K)] + f[1 + j, 1 + i, pl.ds(PAD + 1, K)])
        old = g[1 + j, 1 + i, kk]
        return (2.0 * centre - old) + speed[j, i] * (total - 6.0 * centre)

    def sum_up(value, j, i):
        mean = jnp.sum(value, axis=0, keepdims=True) * (1.0 / K)
        away = value - mean
        stats[slab, 0, j, pl.ds(i, 1)] = mean
        stats[slab, 1, j, pl.ds(i, 1)] = jnp.sum(away * away, axis=0, keepdims=True)

    def far_line_but_arriving(s, i):
        f, g = fields[s], fields[(s + 1) % 2]
        centre = f[1 + far, 1 + i, kk]
        total = f[jnp.where(upper_core, far, far + 2), 1 + i, kk]
        total = total + (f[1 + far, i, kk] + f[1 + far, i + 2, kk])
        total = total + (f[1 + far, 1 + i, pl.ds(PAD - 1, K)] + f[1 + far, 1 + i, pl.ds(PAD + 1, K)])
        return (2.0 * centre - g[1 + far, 1 + i, kk]) + speed[far, i] * (total - 6.0 * centre)

    def step_plane(s, cut, j):
        a, n = cut

        @pl.loop(a, a + n, unroll=4 if s == STEPS - 1 else None)
        def _(i):
            value = line(s, j, i)
            if s < STEPS - 1:
                fields[(s + 1) % 2][1 + j, 1 + i, kk] = value
            else:
                last[j, i] = value
                sum_up(value, j, i)

    def step_inside(s, cut):
        @pl.loop(1, J - 1)
        def _(j):
            step_plane(s, cut, j)

    def wait_below(s, cut, when):
        @pl.when(jnp.logical_and(has["rows"][0], when))
        def _():
            z_copy(s, 1, cut).wait_recv()

    def wait_above(s, cut, when):
        @pl.when(jnp.logical_and(has["rows"][1], when))
        def _():
            z_copy(s, 0, cut).wait_recv()

    def step_outside(s, cut, between=None):
        wait_below(s, cut, upper_core)
        wait_above(s, cut, lower_core)
        step_plane(s, cut, J - 1 - far)
        if between is not None:
            between()
            a, n = cut

            @pl.loop(a, a + n)
            def _(i):
                last[far, i] = far_line_but_arriving(s, i)

        wait_below(s, cut, lower_core)
        wait_above(s, cut, upper_core)
        if between is None:
            step_plane(s, cut, far)
        else:
            arrived = jnp.where(upper_core, J + 1, 0)

            @pl.loop(a, a + n, unroll=4)
            def _(i):
                value = last[far, i] + speed[far, i] * fields[s][arrived, 1 + i, kk]
                last[far, i] = value
                sum_up(value, far, i)

    def finish(planes, rows_i):
        @pl.loop(*planes)
        def _(j):
            at = pl.ds(*rows_i)
            means = [stats[b, 0, j, at] for b in range(slabs)]
            mean = sum(means[1:], means[0]) * (1.0 / slabs)
            spread = sum((stats[b, 1, j, at] for b in range(1, slabs)), stats[0, 1, j, at])
            apart = sum(((m - mean) * (m - mean) for m in means[1:]), (means[0] - mean) * (means[0] - mean))
            variance = (spread + K * apart) * (1.0 / (K * slabs))
            lines_out[0, j, at] = mean
            lines_out[1, j, at] = lax.rsqrt(variance + 0.0001)

    load(now_hbm, even, 0, 0).wait()
    for s in range(STEPS):
        for c, cut in enumerate(chunks[s]):
            a, n = cut
            if s == 0:
                start_loads(c + 2)
                wait_loads(c)
            if c == 0:
                wait_sides("slabs", lambda side: y_copy(s, side))

                @pl.when(has["cols"][0])
                def _():
                    x_copy(s, 1).wait_recv()
            if a + n == I:
                @pl.when(has["cols"][1])
                def _():
                    x_copy(s, 0).wait_recv()
            if s == 1 and c < slabs - 2:
                hear(c)
                if c + 1 < slabs - 2:
                    tell(c + 1)
            if s < STEPS - 1:
                step_outside(s, cut)
                step_inside(s, cut)
                for later in chunks[s + 1]:
                    if a <= later[0] < a + n:
                        for_sides("rows", lambda side: z_copy(s + 1, side, later).start())
                if c == 0:
                    @pl.when(has["cols"][0])
                    def _():
                        x_copy(s + 1, 0).start()
                if a + n == I:
                    @pl.when(has["cols"][1])
                    def _():
                        x_copy(s + 1, 1).start()

                    for_sides("slabs", lambda side: y_copy(s + 1, side).start())
            else:
                step_inside(s, cut)
                if cut != chunks[s][-1]:
                    step_outside(s, cut)
                    send_sums(early, pl.ds(0, J), cut)
                else:
                    nearer = pl.ds(jnp.where(upper_core, 0, 1), J - 1)
                    step_outside(s, cut, lambda: send_sums(early, nearer, cut))
                    send_sums(late, pl.ds(far, 1), cut)

    tail = chunks[-1][-1]
    eight = pl.ds(0, 8)
    soon = even.at[0, pl.ds(0, 2 * (J * I - tail[1]) // 8), eight]
    for d in range(1, slabs):
        pltpu.make_async_remote_copy(
            soon, soon, s_send, s_recv.at[early, d - 1],
            device_id={"slabs": lax.rem(slab + d, slabs)}, device_id_type=MESH).wait_recv()
    finish((0, J), (0, tail[0]))
    finish((jnp.where(upper_core, 0, 1), jnp.where(upper_core, J - 1, J)), tail)
    def all_left(ref, send, axis, side):
        pltpu.make_async_remote_copy(
            ref, ref, send, s_recv.at[0, 0],
            device_id={axis: beside[axis][side]}, device_id_type=MESH).wait_send()

    for_sides("rows", lambda side: all_left(speed.at[pl.ds(0, STEPS)], z_send.at[side], "rows", side))
    for_sides("cols", lambda side: all_left(speed.at[:, pl.ds(0, STEPS)], x_send.at[side], "cols", side))
    for_sides("slabs", lambda side: all_left(speed.at[:, :, pl.ds(0, STEPS)], y_send.at[side], "slabs", side))
    pltpu.make_async_remote_copy(
        stats.at[pl.ds(0, slabs - 1)], stats.at[pl.ds(0, slabs - 1)], s_send, s_recv.at[0, 0],
        device_id={"slabs": lax.rem(slab + 1, slabs)}, device_id_type=MESH).wait_send()

    for d in range(1, slabs):
        s_copy(late, d, pl.ds(far, 1), tail).wait_recv()
    finish((far, far + 1), tail)


def write_kernel(shape, pieces, last, lines, scaled_hbm, end_hbm, scaled, sems):
    J, I, K, M = shape
    n = I // pieces

    @pl.loop(0, pieces)
    def _(c):
        span = pl.ds(c * n, n)
        pltpu.make_async_copy(last.at[:, span], end_hbm.at[:, span], sems.at[0]).start()

    @pl.loop(0, pieces)
    def _(c):
        @pl.loop(0, n)
        def _(r):
            i = c * n + r
            for j in range(J):
                at = pl.ds(i, 1)
                scaled[j, i] = (last[j, i] - lines[0, j, at]) * lines[1, j, at]

        span = pl.ds(c * n, n)
        pltpu.make_async_copy(scaled.at[:, span], scaled_hbm.at[:, span], sems.at[1]).start()

    pltpu.make_async_copy(last, end_hbm, sems.at[0]).wait()
    pltpu.make_async_copy(scaled, scaled_hbm, sems.at[1]).wait()


def shards(sizes, field_now, earlier, speed_square):
    shape = field_now.shape
    J, I, K, M = shape
    slabs = sizes[2]
    hbm = pl.BlockSpec(memory_space=pltpu.HBM)
    vmem = pl.BlockSpec(memory_space=pltpu.VMEM)
    dma = pltpu.SemaphoreType.DMA
    padded = pltpu.VMEM((J + 2, I + 2, K + 2 * PAD, M), F32)
    arrivals = len(chunks_of(I, 1)) + len(chunks_of(I, STEPS - 1))
    last, lines = pl.pallas_call(
        functools.partial(march_kernel, shape, sizes),
        out_shape=(pltpu.VMEM(shape, F32), pltpu.VMEM((2, J, I, M), F32)),
        in_specs=[hbm, hbm, hbm],
        out_specs=(vmem, vmem),
        scratch_shapes=[
            padded,
            padded,
            pltpu.VMEM(shape, F32),
            pltpu.VMEM((slabs, 2, J, I, M), F32),
            dma((2 * len(chunks_of(I, 0)),)),
            dma((2,)),
            dma((2, arrivals)),
            dma((2,)),
            dma((2, 2)),
            dma((2,)),
            dma((2, 2)),
            dma,
            dma((2, slabs - 1)),
            pltpu.SemaphoreType.REGULAR,
            pltpu.SemaphoreType.REGULAR((slabs - 2,)),
        ],
        compiler_params=pltpu.CompilerParams(
            collective_id=0, has_side_effects=True, vmem_limit_bytes=44 * 2**20
        ),
        name="march",
    )(field_now, earlier, speed_square)
    return pl.pallas_call(
        functools.partial(write_kernel, shape, 16),
        out_shape=(jax.ShapeDtypeStruct(shape, F32), jax.ShapeDtypeStruct(shape, F32)),
        in_specs=[vmem, vmem],
        out_specs=(hbm, hbm),
        scratch_shapes=[pltpu.VMEM(shape, F32), dma((2,))],
        compiler_params=pltpu.CompilerParams(vmem_limit_bytes=12 * 2**20),
        name="write",
    )(last, lines)


def solution(mesh):
    placed = P("rows", "cols", "slabs", None)
    sizes = tuple(mesh.shape[a] for a in ("rows", "cols", "slabs"))
    return jax.shard_map(
        functools.partial(shards, sizes),
        mesh=mesh,
        in_specs=(placed, placed, placed),
        out_specs=(placed, placed),
        check_vma=False,
    )
```

```python
import functools

import jax
import jax.numpy as jnp
from jax import lax
from jax.experimental import pallas as pl
from jax.experimental.pallas import tpu as pltpu
from jax.sharding import PartitionSpec as P

STEPS = 3
PAD = 8
MESH = pl.DeviceIdType.MESH
F32 = jnp.float32


def chunks_of(rows, step):
    half = rows // 2
    cut = [(0, half), (half, half)]
    if step == STEPS - 1:
        cut = [(0, half), (half, half // 2), (half + half // 2, half // 4), (half + 3 * half // 4, half // 4)]
    return cut


def march_kernel(
    shape, sizes, now_hbm, before_hbm, speed_hbm,
    last, lines_out,
    even, odd, speed, stats,
    load_sem, z_send, z_recv, x_send, x_recv, y_send, y_recv, s_send, s_recv,
    passed_on, further,
):
    J, I, K, M = shape
    rows, cols, slabs = sizes
    row, col, slab = (lax.axis_index(a) for a in ("rows", "cols", "slabs"))
    has = {
        "rows": (row > 0, row < rows - 1),
        "cols": (col > 0, col < cols - 1),
        "slabs": (slab > 0, slab < slabs - 1),
    }
    beside = {
        "rows": (row - 1, row + 1),
        "cols": (col - 1, col + 1),
        "slabs": (slab - 1, slab + 1),
    }
    upper_core = lax.rem(row, 2) == 1
    jj, ii, kk = pl.ds(1, J), pl.ds(1, I), pl.ds(PAD, K)
    fields = (even, odd, even)
    chunks = [chunks_of(I, s) for s in range(STEPS)]
    slot = [{cut: n for n, cut in enumerate(chunks[s])} for s in range(STEPS)]
    base = [(s % 2) * len(chunks[-1]) for s in range(STEPS)]

    def z_copy(s, side, cut):
        f = fields[s]
        a, n = cut
        edge = 0 if side == 0 else J - 1
        src = now_hbm.at[edge, pl.ds(a, n)] if s == 0 else f.at[1 + edge, pl.ds(1 + a, n), kk]
        dst = f.at[J + 1 if side == 0 else 0, pl.ds(1 + a, n), kk]
        return pltpu.make_async_remote_copy(
            src, dst, z_send.at[side], z_recv.at[side, base[s] + slot[s][cut]],
            device_id={"rows": beside["rows"][side]}, device_id_type=MESH)

    def x_copy(s, side):
        f = fields[s]
        edge = 0 if side == 0 else I - 1
        src = now_hbm.at[:, edge] if s == 0 else f.at[jj, 1 + edge, kk]
        dst = f.at[jj, I + 1 if side == 0 else 0, kk]
        return pltpu.make_async_remote_copy(
            src, dst, x_send.at[side], x_recv.at[s % 2, side],
            device_id={"cols": beside["cols"][side]}, device_id_type=MESH)

    def y_copy(s, side):
        f = fields[s]
        edge = 0 if side == 0 else K - 1
        src = now_hbm.at[:, :, pl.ds(edge, 1)] if s == 0 else f.at[jj, ii, pl.ds(PAD + edge, 1)]
        dst = f.at[jj, ii, pl.ds(PAD + K if side == 0 else PAD - 1, 1)]
        return pltpu.make_async_remote_copy(
            src, dst, y_send.at[side], y_recv.at[s % 2, side],
            device_id={"slabs": beside["slabs"][side]}, device_id_type=MESH)

    far = jnp.where(upper_core, J - 1, 0)
    early, late = 0, 1

    def s_copy(part, d, planes, cut):
        ref = stats.at[slab, :, planes, pl.ds(*cut)]
        return pltpu.make_async_remote_copy(
            ref, ref, s_send, s_recv.at[part, d - 1],
            device_id={"slabs": lax.rem(slab + d, slabs)}, device_id_type=MESH)

    def send_sums(part, planes, cut):
        for d in range(1, slabs):
            s_copy(part, d, planes, cut).start()

    def load(ref, buffer, c, sem):
        a, n = chunks[0][c]
        start = 1 if buffer is not speed else 0
        planes = jj if buffer is not speed else pl.ds(0, J)
        width = kk if buffer is not speed else pl.ds(0, K)
        return pltpu.make_async_copy(
            ref.at[:, pl.ds(a, n)], buffer.at[planes, pl.ds(start + a, n), width], load_sem.at[sem])

    count = len(chunks[0])

    def start_loads(c):
        if c + 1 < count:
            load(now_hbm, even, c + 1, c + 1).start()
        if c < count:
            load(before_hbm, odd, c, count + c).start()
            load(speed_hbm, speed, c, count + c).start()

    def wait_loads(c):
        if c + 1 < count:
            load(now_hbm, even, c + 1, c + 1).wait()
        amount = pl.ds(0, 2 * chunks[0][c][1])
        pltpu.make_async_copy(speed_hbm.at[:, amount], speed.at[:, amount], load_sem.at[count + c]).wait()

    def for_sides(axis, act):
        for side in (0, 1):
            @pl.when(has[axis][side])
            def _():
                act(side)

    def wait_sides(axis, copy):
        for side in (0, 1):
            @pl.when(has[axis][1 - side])
            def _():
                copy(side).wait_recv()

    lower_core = jnp.logical_not(upper_core)
    around = [(axis, side) for axis in ("cols", "slabs") for side in (0, 1)]

    def number(places):
        return sum((has[axis][side].astype(jnp.int32) for axis, side in places), jnp.int32(0))

    def greet(sem, axis, side, when):
        @pl.when(jnp.logical_and(has[axis][side], when))
        def _():
            pl.semaphore_signal(sem, inc=1, device_id={axis: beside[axis][side]}, device_id_type=MESH)

    barrier = pltpu.get_barrier_semaphore()
    for side in (0, 1):
        greet(barrier, "rows", side, True)
    for axis, side in around:
        greet(barrier, axis, side, upper_core)
    load(now_hbm, even, 0, 0).start()
    start_loads(0)
    pl.semaphore_wait(barrier, number([("rows", 0), ("rows", 1)]) + jnp.where(upper_core, number(around), 0))
    for cut in chunks[0]:
        for_sides("rows", lambda side: z_copy(0, side, cut).start())
    for axis, side in around:
        greet(passed_on, axis, side, upper_core)
    pl.semaphore_wait(passed_on, jnp.where(upper_core, number(around), 1))

    @pl.when(upper_core)
    def _():
        pl.semaphore_signal(passed_on, inc=1, device_id={"rows": row - 1}, device_id_type=MESH)

    for_sides("slabs", lambda side: y_copy(0, side).start())
    for_sides("cols", lambda side: x_copy(0, side).start())
    start_loads(1)

    def tell(t):
        for side in (0, 1):
            greet(further.at[t], "slabs", side, True)

    def hear(t):
        pl.semaphore_wait(further.at[t], number([("slabs", 0), ("slabs", 1)]))

    tell(0)

    for f in (even, odd):
        for side, (z, x, y) in enumerate(((0, 0, PAD - 1), (J + 1, I + 1, PAD + K))):
            @pl.when(jnp.logical_not(has["rows"][side]))
            def _():
                @pl.loop(0, I)
                def _(i):
                    f[z, 1 + i, kk] = jnp.zeros((K, M), F32)

            @pl.when(jnp.logical_not(has["cols"][side]))
            def _():
                @pl.loop(0, J)
                def _(j):
                    f[1 + j, x, kk] = jnp.zeros((K, M), F32)

            @pl.when(jnp.logical_not(has["slabs"][side]))
            def _():
                @pl.loop(0, I)
                def _(i):
                    for j in range(J):
                        f[1 + j, 1 + i, pl.ds(y, 1)] = jnp.zeros((1, M), F32)

    def line(s, j, i):
        f, g = fields[s], fields[(s + 1) % 2]
        centre = f[1 + j, 1 + i, kk]
        total = f[j, 1 + i, kk] + f[j + 2, 1 + i, kk]
        total = total + (f[1 + j, i, kk] + f[1 + j, i + 2, kk])
        total = total + (f[1 + j, 1 + i, pl.ds(PAD - 1, K)] + f[1 + j, 1 + i, pl.ds(PAD + 1, K)])
        old = g[1 + j, 1 + i, kk]
        return (2.0 * centre - old) + speed[j, i] * (total - 6.0 * centre)

    def sum_up(value, j, i):
        mean = jnp.sum(value, axis=0, keepdims=True) * (1.0 / K)
        away = value - mean
        stats[slab, 0, j, pl.ds(i, 1)] = mean
        stats[slab, 1, j, pl.ds(i, 1)] = jnp.sum(away * away, axis=0, keepdims=True)

    def far_line_but_arriving(s, i):
        f, g = fields[s], fields[(s + 1) % 2]
        centre = f[1 + far, 1 + i, kk]
        total = f[jnp.where(upper_core, far, far + 2), 1 + i, kk]
        total = total + (f[1 + far, i, kk] + f[1 + far, i + 2, kk])
        total = total + (f[1 + far, 1 + i, pl.ds(PAD - 1, K)] + f[1 + far, 1 + i, pl.ds(PAD + 1, K)])
        return (2.0 * centre - g[1 + far, 1 + i, kk]) + speed[far, i] * (total - 6.0 * centre)

    def step_plane(s, cut, j):
        a, n = cut

        @pl.loop(a, a + n, unroll=4 if s == STEPS - 1 else None)
        def _(i):
            value = line(s, j, i)
            if s < STEPS - 1:
                fields[(s + 1) % 2][1 + j, 1 + i, kk] = value
            else:
                last[j, i] = value
                sum_up(value, j, i)

    def step_inside(s, cut):
        @pl.loop(1, J - 1)
        def _(j):
            step_plane(s, cut, j)

    def wait_below(s, cut, when):
        @pl.when(jnp.logical_and(has["rows"][0], when))
        def _():
            z_copy(s, 1, cut).wait_recv()

    def wait_above(s, cut, when):
        @pl.when(jnp.logical_and(has["rows"][1], when))
        def _():
            z_copy(s, 0, cut).wait_recv()

    def step_outside(s, cut, between=None):
        wait_below(s, cut, upper_core)
        wait_above(s, cut, lower_core)
        step_plane(s, cut, J - 1 - far)
        if between is not None:
            between()
            a, n = cut

            @pl.loop(a, a + n)
            def _(i):
                last[far, i] = far_line_but_arriving(s, i)

        wait_below(s, cut, lower_core)
        wait_above(s, cut, upper_core)
        if between is None:
            step_plane(s, cut, far)
        else:
            arrived = jnp.where(upper_core, J + 1, 0)

            @pl.loop(a, a + n, unroll=4)
            def _(i):
                value = last[far, i] + speed[far, i] * fields[s][arrived, 1 + i, kk]
                last[far, i] = value
                sum_up(value, far, i)

    def finish(planes, rows_i):
        @pl.loop(*planes)
        def _(j):
            at = pl.ds(*rows_i)
            means = [stats[b, 0, j, at] for b in range(slabs)]
            mean = sum(means[1:], means[0]) * (1.0 / slabs)
            spread = sum((stats[b, 1, j, at] for b in range(1, slabs)), stats[0, 1, j, at])
            apart = sum(((m - mean) * (m - mean) for m in means[1:]), (means[0] - mean) * (means[0] - mean))
            variance = (spread + K * apart) * (1.0 / (K * slabs))
            lines_out[0, j, at] = mean
            lines_out[1, j, at] = lax.rsqrt(variance + 0.0001)

    load(now_hbm, even, 0, 0).wait()
    for s in range(STEPS):
        for c, cut in enumerate(chunks[s]):
            a, n = cut
            if s == 0:
                start_loads(c + 2)
                wait_loads(c)
            if c == 0:
                wait_sides("slabs", lambda side: y_copy(s, side))

                @pl.when(has["cols"][0])
                def _():
                    x_copy(s, 1).wait_recv()
            if a + n == I:
                @pl.when(has["cols"][1])
                def _():
                    x_copy(s, 0).wait_recv()
            if s == 1 and c < slabs - 2:
                hear(c)
                if c + 1 < slabs - 2:
                    tell(c + 1)
            if s < STEPS - 1:
                step_outside(s, cut)
                step_inside(s, cut)
                for later in chunks[s + 1]:
                    if a <= later[0] < a + n:
                        for_sides("rows", lambda side: z_copy(s + 1, side, later).start())
                if c == 0:
                    @pl.when(has["cols"][0])
                    def _():
                        x_copy(s + 1, 0).start()
                if a + n == I:
                    @pl.when(has["cols"][1])
                    def _():
                        x_copy(s + 1, 1).start()

                    for_sides("slabs", lambda side: y_copy(s + 1, side).start())
            else:
                step_inside(s, cut)
                if cut != chunks[s][-1]:
                    step_outside(s, cut)
                    send_sums(early, pl.ds(0, J), cut)
                else:
                    nearer = pl.ds(jnp.where(upper_core, 0, 1), J - 1)
                    step_outside(s, cut, lambda: send_sums(early, nearer, cut))
                    send_sums(late, pl.ds(far, 1), cut)

    tail = chunks[-1][-1]
    eight = pl.ds(0, 8)
    soon = even.at[0, pl.ds(0, 2 * (J * I - tail[1]) // 8), eight]
    for d in range(1, slabs):
        pltpu.make_async_remote_copy(
            soon, soon, s_send, s_recv.at[early, d - 1],
            device_id={"slabs": lax.rem(slab + d, slabs)}, device_id_type=MESH).wait_recv()
    finish((0, J), (0, tail[0]))
    finish((jnp.where(upper_core, 0, 1), jnp.where(upper_core, J - 1, J)), tail)
    def all_left(ref, send, axis, side):
        pltpu.make_async_remote_copy(
            ref, ref, send, s_recv.at[0, 0],
            device_id={axis: beside[axis][side]}, device_id_type=MESH).wait_send()

    for_sides("rows", lambda side: all_left(speed.at[pl.ds(0, STEPS)], z_send.at[side], "rows", side))
    for_sides("cols", lambda side: all_left(speed.at[:, pl.ds(0, STEPS)], x_send.at[side], "cols", side))
    for_sides("slabs", lambda side: all_left(speed.at[:, :, pl.ds(0, STEPS)], y_send.at[side], "slabs", side))
    pltpu.make_async_remote_copy(
        stats.at[pl.ds(0, slabs - 1)], stats.at[pl.ds(0, slabs - 1)], s_send, s_recv.at[0, 0],
        device_id={"slabs": lax.rem(slab + 1, slabs)}, device_id_type=MESH).wait_send()

    for d in range(1, slabs):
        s_copy(late, d, pl.ds(far, 1), tail).wait_recv()
    finish((far, far + 1), tail)


def write_kernel(shape, pieces, last, lines, scaled_hbm, end_hbm, scaled, sems):
    J, I, K, M = shape
    n = I // pieces

    @pl.loop(0, pieces)
    def _(c):
        span = pl.ds(c * n, n)
        pltpu.make_async_copy(last.at[:, span], end_hbm.at[:, span], sems.at[0]).start()

    @pl.loop(0, pieces)
    def _(c):
        @pl.loop(0, n)
        def _(r):
            i = c * n + r
            for j in range(J):
                at = pl.ds(i, 1)
                scaled[j, i] = (last[j, i] - lines[0, j, at]) * lines[1, j, at]

        span = pl.ds(c * n, n)
        pltpu.make_async_copy(scaled.at[:, span], scaled_hbm.at[:, span], sems.at[1]).start()

    pltpu.make_async_copy(last, end_hbm, sems.at[0]).wait()
    pltpu.make_async_copy(scaled, scaled_hbm, sems.at[1]).wait()


def shards(sizes, field_now, earlier, speed_square):
    shape = field_now.shape
    J, I, K, M = shape
    slabs = sizes[2]
    hbm = pl.BlockSpec(memory_space=pltpu.HBM)
    vmem = pl.BlockSpec(memory_space=pltpu.VMEM)
    dma = pltpu.SemaphoreType.DMA
    padded = pltpu.VMEM((J + 2, I + 2, K + 2 * PAD, M), F32)
    arrivals = len(chunks_of(I, 1)) + len(chunks_of(I, STEPS - 1))
    last, lines = pl.pallas_call(
        functools.partial(march_kernel, shape, sizes),
        out_shape=(pltpu.VMEM(shape, F32), pltpu.VMEM((2, J, I, M), F32)),
        in_specs=[hbm, hbm, hbm],
        out_specs=(vmem, vmem),
        scratch_shapes=[
            padded,
            padded,
            pltpu.VMEM(shape, F32),
            pltpu.VMEM((slabs, 2, J, I, M), F32),
            dma((2 * len(chunks_of(I, 0)),)),
            dma((2,)),
            dma((2, arrivals)),
            dma((2,)),
            dma((2, 2)),
            dma((2,)),
            dma((2, 2)),
            dma,
            dma((2, slabs - 1)),
            pltpu.SemaphoreType.REGULAR,
            pltpu.SemaphoreType.REGULAR((slabs - 2,)),
        ],
        compiler_params=pltpu.CompilerParams(
            collective_id=0, has_side_effects=True, vmem_limit_bytes=44 * 2**20
        ),
        name="march",
    )(field_now, earlier, speed_square)
    return pl.pallas_call(
        functools.partial(write_kernel, shape, 8),
        out_shape=(jax.ShapeDtypeStruct(shape, F32), jax.ShapeDtypeStruct(shape, F32)),
        in_specs=[vmem, vmem],
        out_specs=(hbm, hbm),
        scratch_shapes=[pltpu.VMEM(shape, F32), dma((2,))],
        compiler_params=pltpu.CompilerParams(vmem_limit_bytes=12 * 2**20),
        name="write",
    )(last, lines)


def solution(mesh):
    placed = P("rows", "cols", "slabs", None)
    sizes = tuple(mesh.shape[a] for a in ("rows", "cols", "slabs"))
    return jax.shard_map(
        functools.partial(shards, sizes),
        mesh=mesh,
        in_specs=(placed, placed, placed),
        out_specs=(placed, placed),
        check_vma=False,
    )
```
